32 devices in a mesh: seq: 4 (over x, core), vocab: 8 (over z, y).
Axes of the slice: x: 2, y: 2, z: 4, core: 2. Of those that a mesh axis runs over, the one named last changes fastest.
Arguments:
- hidden: bfloat16 [512, 4608], P('seq', 'vocab'), may hold values from -6 to 6
- norm_gain: float32 [4608], replicated, may hold values from -1.5 to 1.5
- unembed: bfloat16 [256000, 4608], P(('seq', 'vocab')), may hold values from -0.375 to 0.375
- targets: int32 [512], P('seq'), may hold values from 0 to 255999
Outputs:
- log_prob: float32 [512], P('seq')
- entropy: float32 [512], P('seq')
The draws below stay inside these ranges and needn't reach their ends.
All inputs are finite; a program needn't handle non-finite values.
Results may differ from the reference program's by a relative error of at most 0.0012.
Values may be sent and summed in bfloat16 or wider, within the bound.
A program may use at most 128 MiB of HBM per device.

```python
import jax
import jax.numpy as jnp
from jax import lax

D = 4608
VOCAB = 256000
TOKENS = 512


def touch_ends(values, stream_key, low, top_value):
    longest = values.shape.index(max(values.shape))
    spots = []
    for shift in (0, 1):
        where = [jax.random.randint(jax.random.fold_in(stream_key, axis), (), 0, length) for axis, length in enumerate(values.shape)]
        where[longest] = (where[longest] + shift) % values.shape[longest]
        spots.append(tuple(where))
    return values.at[spots[0]].set(low).at[spots[1]].set(top_value)


def block_levels(key, extent, split, least, largest):
    level = 1.0
    for dim, blocks in split:
        heights = jax.random.uniform(jax.random.fold_in(jax.random.fold_in(key, 6), dim), (blocks,), jnp.float32, least / len(split), largest / len(split))
        level = level * jnp.repeat(jnp.exp(heights), extent[dim] // blocks).reshape((-1,) + (1,) * (len(extent) - 1 - dim))
    return level


def centred(rng, dims, spread, reach, pieces=(), kind=jnp.bfloat16):
    result = spread * jax.random.normal(rng, dims, jnp.float32)
    if pieces:
        result = result * block_levels(rng, dims, pieces, -0.22, 0.18)
    return jnp.clip(result, -reach, reach).astype(kind)


def setup_inputs(seed: int = 0) -> dict:
    splits = jax.random.split(jax.random.key(seed), 5)
    return {
        "hidden": centred(splits[0], (TOKENS, D), 1.0, 6.0, ((0, 4), (1, 8))),
        "norm_gain": centred(splits[1], (D,), 0.3, 1.5, (), jnp.float32),
        "unembed": centred(splits[2], (VOCAB, D), (D // 16) ** -0.5, 0.375, ((0, 32),)),
        "targets": touch_ends(jax.random.randint(splits[3], (TOKENS,), 0, VOCAB), jax.random.fold_in(splits[3], 1), 0, VOCAB - 1).astype(jnp.int32),
    }


softcap = 30.0
epsilon = 1e-06

def normalize(hidden, norm_gain):
    values = hidden.astype(jnp.float32)
    scale = lax.rsqrt(lax.optimization_barrier(jnp.mean(values * values, axis=1, keepdims=True)) + epsilon)
    return (values * scale * (1.0 + norm_gain.astype(jnp.float32))).astype(jnp.bfloat16)

def reference(hidden, norm_gain, unembed, targets):
    normed = normalize(hidden, norm_gain)
    blocks = unembed.reshape(32, VOCAB // 32, D)

    def block_sums(block):
        logits = lax.dot_general(normed, block, (((1,), (1,)), ((), ())), preferred_element_type=jnp.float32)
        capped = softcap * jnp.tanh(logits / softcap)
        weights = jnp.exp(capped - softcap)
        return (lax.optimization_barrier(jnp.sum(weights, axis=1)), lax.optimization_barrier(jnp.sum(weights * capped, axis=1)))
    sums, moments = lax.map(block_sums, blocks)
    total = lax.optimization_barrier(jnp.sum(sums, axis=0))
    moment = lax.optimization_barrier(jnp.sum(moments, axis=0))
    picked = unembed[targets.astype(jnp.int32)].astype(jnp.float32)
    target_logit = lax.optimization_barrier(jnp.sum(normed.astype(jnp.float32) * picked, axis=1))
    chosen = softcap * jnp.tanh(target_logit / softcap)
    log_norm = softcap + jnp.log(total)
    return (chosen - log_norm, log_norm - moment / total)
```

```python
import functools

import jax
import jax.numpy as jnp
from jax import lax
from jax.experimental import pallas as pl
from jax.experimental.pallas import tpu as pltpu
from jax.sharding import PartitionSpec as P

softcap = 30.0
epsilon = 1e-06
log2e = 1.4426950408889634
CORES = 2
LANES = 128
DEPTH = 256
SLOTS = 3
MESH = pl.DeviceIdType.MESH


def divisor(extent, most):
    return max(n for n in range(16, most + 1, 16) if extent % n == 0)


def plan(stages, chunk):
    whole = chunk // DEPTH * DEPTH
    passes = [[(0, 0, whole)]]
    if stages > 1:
        passes.append([(0, whole, chunk - whole), (1, 0, chunk)])
    elif whole < chunk:
        passes.append([(0, whole, chunk - whole)])
    if stages > 2:
        passes.append([(k, 0, chunk) for k in range(2, stages)])
    return [[piece for piece in part if piece[2]] for part in passes]


def head_kernel(sizes, tile, sub, hidden_ref, gain_ref, targets_ref, unembed_ref, out_ref,
                held, gains, normed, partial, scales, all_targets, weights, logits, sums,
                stats, arrived, sems, weight_sem):
    X, Y, Z = sizes["x"], sizes["y"], sizes["z"]
    seq, vocab = lax.axis_index("seq"), lax.axis_index("vocab")
    core = lax.rem(seq, CORES)
    x, y, z = seq // CORES, lax.rem(vocab, Y), vocab // Y
    seqs, vocabs = X * CORES, Z * Y
    count = seqs * vocabs
    me = seq * vocabs + vocab
    part, own = held.shape[4], held.shape[5]
    chunk, width, tokens = Y * part, Z * Y * part, seqs * own
    rows = unembed_ref.shape[0]
    tiles = rows // tile
    passes = plan(Z, chunk)
    total_steps = len(passes) * tiles

    def place(k):
        other = lax.rem(me + k, count)
        return other, {"seq": other // vocabs, "vocab": lax.rem(other, vocabs)}

    def device(dx=0, dy=0, dz=0, dc=0):
        return {
            "seq": lax.rem(x + dx, X) * CORES + lax.rem(core + dc, CORES),
            "vocab": lax.rem(z + dz, Z) * Y + lax.rem(y + dy, Y),
        }

    def level(k):
        return lax.rem(z - k + Z, Z)

    barrier = pltpu.get_barrier_semaphore()

    def greet(k, _):
        pl.semaphore_signal(barrier, inc=1, device_id=place(k)[1], device_id_type=MESH)
        return 0

    lax.fori_loop(1, count, greet, 0)

    def fetches(p, i, slot):
        start, out = 0, []
        row = pl.ds(pl.multiple_of(i * tile, tile), tile)
        for n, (k, first, length) in enumerate(passes[p]):
            column = pl.multiple_of(level(k) * chunk + first, LANES)
            out.append(pltpu.make_async_copy(
                unembed_ref.at[row, pl.ds(column, length)],
                weights.at[slot, :, pl.ds(start, length)],
                weight_sem.at[slot, n],
            ))
            start += length
        return out

    for g in range(min(SLOTS - 1, total_steps)):
        for copy in fetches(g // tiles, g % tiles, g % SLOTS):
            copy.start()

    squares = jnp.zeros((1, own), jnp.float32)
    for a in range(0, part, LANES):
        b = min(a + LANES, part)
        values = jnp.transpose(hidden_ref[:, a:b].astype(jnp.float32))
        squares += jnp.sum(values * values, axis=0, keepdims=True)
        held[core, z, x, y, a:b, :] = values.astype(jnp.bfloat16)
    partial[me] = squares
    all_targets[seq] = targets_ref[...]
    pl.semaphore_wait(barrier, count - 1)

    def remote(src, dst, name, index, to):
        return pltpu.make_async_remote_copy(
            src_ref=src, dst_ref=dst, send_sem=sems[name].at[(0,) + index],
            recv_sem=sems[name].at[(1,) + index], device_id=to, device_id_type=MESH,
        )

    def square_copy(k, slot):
        return remote(partial.at[slot], partial.at[slot], "square", (k,), place(k)[1])

    def target_copy(k, slot):
        return remote(targets_ref, all_targets.at[slot], "target", (k,),
                      {"seq": lax.rem(seq + k, seqs), "vocab": vocab})

    peers = sorted(
        ((dx, dy) for dx in range(X) for dy in range(Y) if dx or dy),
        key=lambda d: (d[0] != 0) + (d[1] != 0),
    )

    def plane_copy(k, j, sx, sy):
        block = held.at[core, level(k), sx, sy]
        dx, dy = peers[j]
        return remote(block, block, "plane", (k, j), device(dx=dx, dy=dy))

    def plane_send(k, j):
        return plane_copy(k, j, x, y)

    def plane_recv(k, j):
        dx, dy = peers[j]
        return plane_copy(k, j, lax.rem(x - dx + X, X), lax.rem(y - dy + Y, Y))

    def column_copy(k, level_):
        block = held.at[core, level_, x, y]
        return remote(block, block, "column", (k,), device(dz=k))

    def pair_copy(k, j, mine):
        dx, dy = (0, 0) if j == len(peers) else peers[j]
        c = core if mine else 1 - core
        block = held.at[c, level(k), lax.rem(x - dx + X, X), lax.rem(y - dy + Y, Y)]
        return remote(block, block, "pair", (k, j), device(dc=1))

    def send_square(k, _):
        square_copy(k, me).start()
        return 0

    lax.fori_loop(1, count, send_square, 0)
    for k in range(1, seqs):
        target_copy(k, seq).start()

    def spread(k):
        for j in range(len(peers)):
            plane_send(k, j).start()
        pair_copy(k, len(peers), True).start()

    def column_arrived(k):
        column_copy(k, level(k)).wait_recv()
        spread(k)

    def plane_arrived(k):
        for j in range(len(peers)):
            plane_recv(k, j).wait_recv()
            pair_copy(k, j, True).start()

    def pair_arrived(k):
        for j in range(len(peers) + 1):
            pair_copy(k, j, False).wait_recv()

    spread(0)
    for k in range(1, Z):
        column_copy(k, z).start()

    lanes = width // LANES
    columns = jnp.transpose(jnp.concatenate(
        [1.0 + gain_ref[...], jnp.zeros((LANES - lanes, LANES), jnp.float32)], axis=0
    ))
    for j in range(lanes):
        gains[j * LANES:(j + 1) * LANES, :] = jnp.broadcast_to(columns[:, j:j + 1], (LANES, LANES))

    def square_arrived(k, _):
        square_copy(k, place(count - k)[0]).wait_recv()
        return 0

    lax.fori_loop(1, count, square_arrived, 0)
    for s in range(seqs):
        squares = partial[s * vocabs]
        for v in range(1, vocabs):
            squares = squares + partial[s * vocabs + v]
        scales[s] = lax.rsqrt(squares / width + epsilon)
    for k in range(1, seqs):
        target_copy(k, lax.rem(seq - k + seqs, seqs)).wait_recv()

    def normalize(k):
        for s in range(seqs):
            for v in range(Y):
                block = held[s % CORES, level(k), s // CORES, v].astype(jnp.float32)
                start = pl.multiple_of(level(k) * chunk + v * part, 16)
                at = k * chunk + v * part
                normed[at:at + part, s * own:(s + 1) * own] = (
                    block * scales[s] * gains[pl.ds(start, part), :]
                ).astype(jnp.bfloat16)

    plane_arrived(0)
    pair_arrived(0)
    normalize(0)

    ids = jnp.concatenate([all_targets[s] for s in range(seqs)], axis=1) - me * rows
    lines = lax.broadcasted_iota(jnp.int32, (sub, tokens), 0)
    sums[...] = jnp.zeros_like(sums)

    def fold(values):
        return jnp.sum(values.reshape(sub // 8, 8, tokens), axis=0)

    events = [[] for _ in passes]
    last_pass = len(passes) - 1
    if Z > 1:
        early = [(functools.partial(column_arrived, k)) for k in range(1, Z)]
        for n, event in enumerate(early):
            events[0].append((min(n, tiles - 1), event))
        events[0].append((tiles - 1, functools.partial(plane_arrived, 1)))
        for n, k in enumerate(range(2, Z)):
            events[1].append((min(1 + 2 * n, tiles - 1), functools.partial(plane_arrived, k)))

    base = 0
    for p, pieces in enumerate(passes):
        depth = sum(length for _, _, length in pieces)
        for k in sorted({piece[0] for piece in pieces}):
            if k and pieces[-1][0] >= k and (p == 0 or k not in {q[0] for q in passes[p - 1]}):
                pair_arrived(k)
                normalize(k)

        def step(i, _, p=p, depth=depth, base=base):
            g = p * tiles + i
            slot = lax.rem(g, SLOTS)
            ahead = lax.rem(g + SLOTS - 1, SLOTS)

            def prefetch(q, n):
                for copy in fetches(q, n, ahead):
                    copy.start()

            n = i + SLOTS - 1
            for q in range(p, len(passes)):
                low, high = (q - p) * tiles, (q - p + 1) * tiles
                if low > tiles - 1 + SLOTS - 1 or high <= SLOTS - 1:
                    continue
                pl.when((n >= low) & (n < high))(functools.partial(prefetch, q, n - low))
            for at, event in events[p]:
                pl.when(i == at)(event)
            for copy in fetches(p, i, slot):
                copy.wait()
            if p == last_pass:
                total, moment, chosen = sums[0], sums[1], sums[2]
            for s in range(tile // sub):
                here = pl.ds(pl.multiple_of(i * tile + s * sub, sub), sub)
                value = jnp.dot(
                    weights[slot, s * sub:(s + 1) * sub, 0:depth], normed[base:base + depth, :],
                    preferred_element_type=jnp.float32,
                )
                if p:
                    value = logits[here, :] + value
                if p < last_pass:
                    logits[here, :] = value
                else:
                    squashed = jnp.tanh(value * (1.0 / softcap))
                    weight = jnp.exp2(squashed * (softcap * log2e) - softcap * log2e)
                    hit = lines == ids - (i * tile + s * sub)
                    total = total + fold(weight)
                    moment = moment + fold(weight * squashed)
                    chosen = chosen + fold(jnp.where(hit, squashed, 0.0))
            if p == last_pass:
                sums[0], sums[1], sums[2] = total, moment, chosen
            return 0

        lax.fori_loop(0, tiles, step, 0)
        base += depth

    line = jnp.concatenate([
        jnp.sum(sums[0], axis=0, keepdims=True),
        softcap * jnp.sum(sums[1], axis=0, keepdims=True),
        softcap * jnp.sum(sums[2], axis=0, keepdims=True),
    ], axis=0)
    for s in range(seqs):
        stats[s] = line[:, s * own:(s + 1) * own]
    arrived[me] = stats[seq]

    def square_sent(k, _):
        square_copy(k, me).wait_send()
        return 0

    lax.fori_loop(1, count, square_sent, 0)
    for k in range(1, seqs):
        target_copy(k, seq).wait_send()
    for k in range(Z):
        for j in range(len(peers)):
            plane_send(k, j).wait_send()
            pair_copy(k, j, True).wait_send()
        pair_copy(k, len(peers), True).wait_send()
        if k:
            column_copy(k, z).wait_send()

    def stat_copy(k, slot):
        other, where = place(k)
        return remote(stats.at[other // vocabs], arrived.at[slot], "stat", (k,), where)

    def send_stat(k, _):
        stat_copy(k, me).start()
        return 0

    def stat_arrived(k, _):
        stat_copy(k, place(count - k)[0]).wait_recv()
        return 0

    def stat_sent(k, _):
        stat_copy(k, me).wait_send()
        return 0

    lax.fori_loop(1, count, send_stat, 0)
    lax.fori_loop(1, count, stat_arrived, 0)
    result = arrived[0]
    for i in range(1, count):
        result = result + arrived[i]
    total, moment, chosen = result[0:1], result[1:2], result[2:3]
    log_norm = softcap + jnp.log(total)
    out_ref[0:1, :] = chosen - log_norm
    out_ref[1:2, :] = log_norm - moment / total
    lax.fori_loop(1, count, stat_sent, 0)


def on_device(seqs, vocabs, hidden, norm_gain, unembed, targets):
    rows, width = unembed.shape
    own, part = hidden.shape
    Y = 2 ** ((vocabs.bit_length() - 1) // 2)
    X, Z = seqs // CORES, vocabs // Y
    sizes = {"x": X, "y": Y, "z": Z}
    count = seqs * vocabs
    tokens = seqs * own
    tile = divisor(rows, 1600)
    sub = divisor(tile, 160)
    passes = plan(Z, Y * part)
    deepest = max(sum(length for _, _, length in pieces) for pieces in passes)
    most = max(len(pieces) for pieces in passes)
    planes = X * Y
    dma = pltpu.SemaphoreType.DMA
    vmem = pl.BlockSpec(memory_space=pltpu.VMEM)
    out = pl.pallas_call(
        functools.partial(head_kernel, sizes, tile, sub),
        out_shape=jax.ShapeDtypeStruct((2, own), jnp.float32),
        in_specs=[vmem, vmem, vmem, pl.BlockSpec(memory_space=pltpu.HBM)],
        out_specs=vmem,
        scratch_shapes=[
            pltpu.VMEM((CORES, Z, X, Y, part, own), jnp.bfloat16),
            pltpu.VMEM((width, LANES), jnp.float32),
            pltpu.VMEM((width, tokens), jnp.bfloat16),
            pltpu.VMEM((count, 1, own), jnp.float32),
            pltpu.VMEM((seqs, 1, own), jnp.float32),
            pltpu.VMEM((seqs, 1, own), jnp.int32),
            pltpu.VMEM((SLOTS, tile, deepest), jnp.bfloat16),
            pltpu.VMEM((rows, tokens), jnp.float32),
            pltpu.VMEM((3, 8, tokens), jnp.float32),
            pltpu.VMEM((seqs, 3, own), jnp.float32),
            pltpu.VMEM((count, 3, own), jnp.float32),
            {
                "square": dma((2, count)),
                "target": dma((2, seqs)),
                "plane": dma((2, Z, planes)),
                "column": dma((2, Z)),
                "pair": dma((2, Z, planes)),
                "stat": dma((2, count)),
            },
            dma((SLOTS, most)),
        ],
        compiler_params=pltpu.CompilerParams(
            collective_id=0, has_side_effects=True, vmem_limit_bytes=67000000
        ),
        name="head",
    )(hidden, norm_gain.reshape(width // LANES, LANES), targets.reshape(1, own), unembed)
    return out[0], out[1]


def solution(mesh):
    return jax.shard_map(
        functools.partial(on_device, mesh.shape["seq"], mesh.shape["vocab"]),
        mesh=mesh,
        in_specs=(P("seq", "vocab"), P(), P(("seq", "vocab"), None), P("seq")),
        out_specs=(P("seq"), P("seq")),
        check_vma=False,
    )
```

```python
import functools

import jax
import jax.numpy as jnp
from jax import lax
from jax.experimental import pallas as pl
from jax.experimental.pallas import tpu as pltpu
from jax.sharding import PartitionSpec as P

softcap = 30.0
epsilon = 1e-06
log2e = 1.4426950408889634
CORES = 2
LANES = 128
DEPTH = 256
SLOTS = 3
MESH = pl.DeviceIdType.MESH


def divisor(extent, most):
    return max(n for n in range(16, most + 1, 16) if extent % n == 0)


def plan(stages, parts, part):
    chunk = parts * part
    own = part // DEPTH * DEPTH
    if parts == 2 and own and (part - own) % (LANES // 2) == 0:
        passes = [[(0, "own", own)], [(0, "rest", own)]]
        left = [(0, "left", chunk - 2 * own)]
    else:
        own = chunk // DEPTH * DEPTH
        passes = [[(0, "own", own)]]
        left = [(0, "rest", chunk - own)]
    left = [piece for piece in left if piece[2]]
    if stages > 1:
        passes.append(left + [(1, 0, chunk)])
    elif left:
        passes.append(left)
    if stages > 2:
        passes.append([(k, 0, chunk) for k in range(2, stages)])
    return passes


def chunk_gap(passes):
    return sum(piece[2] for pieces in passes for piece in pieces if piece[1] == "left")


def head_kernel(sizes, tile, sub, wide, wide_sub, hidden_ref, gain_hbm, targets_hbm, unembed_ref, out_ref,
                held, gain_ref, targets_ref, gains, normed, partial, scales, all_targets, weights, wides, logits, sums,
                stats, arrived, sems, weight_sem, wide_sem, load_sem):
    X, Y, Z = sizes["x"], sizes["y"], sizes["z"]
    seq, vocab = lax.axis_index("seq"), lax.axis_index("vocab")
    core = lax.rem(seq, CORES)
    x, y, z = seq // CORES, lax.rem(vocab, Y), vocab // Y
    seqs, vocabs = X * CORES, Z * Y
    count = seqs * vocabs
    me = seq * vocabs + vocab
    part, own = held.shape[4], held.shape[5]
    chunk, width, tokens = Y * part, Z * Y * part, seqs * own
    rows = unembed_ref.shape[0]
    passes = plan(Z, Y, part)
    split = [piece[1] for pieces in passes for piece in pieces].count("left") > 0
    halves = 2 if split else 1
    narrow, tiles, broad = passes[halves:], rows // tile, rows // wide
    total_steps = len(narrow) * tiles
    lead = passes[0][0][2]
    rest = chunk - lead

    others = [(a, b) for a in range(seqs) for b in range(vocabs) if a or b]

    def place(a, b):
        return {"seq": lax.rem(seq + a, seqs), "vocab": lax.rem(vocab + b, vocabs)}

    def device(dx=0, dy=0, dz=0, dc=0):
        return {
            "seq": lax.rem(x + dx, X) * CORES + lax.rem(core + dc, CORES),
            "vocab": lax.rem(z + dz, Z) * Y + lax.rem(y + dy, Y),
        }

    def level(k):
        return lax.rem(z - k + Z, Z)

    barrier = pltpu.get_barrier_semaphore()

    loads = [
        pltpu.make_async_copy(src, dst, load_sem.at[n])
        for n, (src, dst) in enumerate((
            (hidden_ref, held.at[core, z, x, y]), (targets_hbm, targets_ref), (gain_hbm, gain_ref)
        ))
    ]
    for load in loads:
        load.start()
    for other in others:
        pl.semaphore_signal(barrier, inc=1, device_id=place(*other), device_id_type=MESH)

    def first_of(kind):
        if not split:
            return {"own": 0, "rest": lead}.get(kind, 0)
        behind = (1 - y) * lead
        return {"own": y * rest, "rest": behind, "left": behind + lead}.get(kind, 0)

    def wide_fetch(p, i):
        column = pl.multiple_of(level(0) * chunk + first_of(passes[p][0][1]), LANES)
        slot = i % wides.shape[0]
        return pltpu.make_async_copy(
            unembed_ref.at[pl.ds(i * wide, wide), pl.ds(column, lead)],
            wides.at[slot], wide_sem.at[slot],
        )

    def fetches(p, i, slot):
        start, out = 0, []
        row = pl.ds(pl.multiple_of(i * tile, tile), tile)
        for n, (k, first, length) in enumerate(narrow[p]):
            column = pl.multiple_of(level(k) * chunk + first_of(first), LANES)
            out.append(pltpu.make_async_copy(
                unembed_ref.at[row, pl.ds(column, length)],
                weights.at[slot, :, pl.ds(start, length)],
                weight_sem.at[slot, n],
            ))
            start += length
        return out

    bulk = [(p, i) for p in range(halves) for i in range(broad)]
    for p, i in bulk[:wides.shape[0]]:
        wide_fetch(p, i).start()
    for g in range(min(SLOTS - 1, total_steps)):
        for copy in fetches(g // tiles, g % tiles, g % SLOTS):
            copy.start()

    for load in loads:
        load.wait()
    all_targets[seq] = targets_ref[...]
    values = held[core, z, x, y].astype(jnp.float32)
    partial[me] = jnp.sum(values * values, axis=0, keepdims=True)
    pl.semaphore_wait(barrier, count - 1)

    def remote(src, dst, name, index, to):
        return pltpu.make_async_remote_copy(
            src_ref=src, dst_ref=dst, send_sem=sems[name].at[(0,) + index],
            recv_sem=sems[name].at[(1,) + index], device_id=to, device_id_type=MESH,
        )

    def square_copy(block, to):
        return remote(block, block, "square", (), to)

    square_all = square_copy(partial.at[pl.ds(0, count - 1)], place(*others[0]))

    def target_copy(k, slot):
        return remote(targets_ref, all_targets.at[slot], "target", (k,),
                      {"seq": lax.rem(seq + k, seqs), "vocab": vocab})

    peers = sorted(
        ((dx, dy) for dx in range(X) for dy in range(Y) if dx or dy),
        key=lambda d: (d[1] != 0, (d[0] != 0) + (d[1] != 0)),
    )

    def plane_copy(k, j, sx, sy):
        block = held.at[core, level(k), sx, sy]
        dx, dy = peers[j]
        return remote(block, block, "plane", (k, j), device(dx=dx, dy=dy))

    def plane_send(k, j):
        return plane_copy(k, j, x, y)

    def plane_recv(k, j):
        dx, dy = peers[j]
        return plane_copy(k, j, lax.rem(x - dx + X, X), lax.rem(y - dy + Y, Y))

    def column_copy(k, level_):
        block = held.at[core, level_, x, y]
        return remote(block, block, "column", (k,), device(dz=k))

    def pair_copy(k, j, mine):
        dx, dy = (0, 0) if j == len(peers) else peers[j]
        c = core if mine else 1 - core
        block = held.at[c, level(k), lax.rem(x - dx + X, X), lax.rem(y - dy + Y, Y)]
        return remote(block, block, "pair", (k, j), device(dc=1))

    for other in others:
        square_copy(partial.at[me], place(*other)).start()
    for k in range(1, seqs):
        target_copy(k, seq).start()

    def spread(k):
        for j in range(len(peers)):
            plane_send(k, j).start()
        pair_copy(k, len(peers), True).start()

    def column_arrived(k):
        column_copy(k, level(k)).wait_recv()
        spread(k)

    near = [j for j, d in enumerate(peers) if d[1] == 0]
    far = [j for j, d in enumerate(peers) if d[1] != 0]

    def plane_arrived(k, which=near + far):
        for j in which:
            plane_recv(k, j).wait_recv()
            pair_copy(k, j, True).start()

    def pair_arrived(k, which=near + far + [len(peers)]):
        for j in which:
            pair_copy(k, j, False).wait_recv()

    spread(0)
    for k in range(1, min(Z, 2)):
        column_copy(k, z).start()

    lanes = width // LANES
    columns = jnp.transpose(jnp.concatenate(
        [1.0 + gain_ref[...], jnp.zeros((LANES - lanes, LANES), jnp.float32)], axis=0
    ))
    for j in range(lanes):
        gains[j * LANES:(j + 1) * LANES, :] = jnp.broadcast_to(columns[:, j:j + 1], (LANES, LANES))

    square_all.wait_recv()
    for s in range(seqs):
        squares = partial[s * vocabs]
        for v in range(1, vocabs):
            squares = squares + partial[s * vocabs + v]
        scales[s] = lax.rsqrt(squares / width + epsilon)
    for k in range(2, min(Z, 3)):
        column_copy(k, z).start()
    for k in range(1, seqs):
        target_copy(k, lax.rem(seq - k + seqs, seqs)).wait_recv()

    gap = 0 if not split else rest - lead

    def normalize(k, offsets=range(Y)):
        for d in offsets:
            v = lax.rem(y + d, Y)
            for s in range(seqs):
                block = held[s % CORES, level(k), s // CORES, v].astype(jnp.float32)
                start = pl.multiple_of(level(k) * chunk + v * part, 16)
                at = pl.multiple_of(k * chunk + (gap if k else 0) + v * part, 16)
                normed[pl.ds(at, part), s * own:(s + 1) * own] = (
                    block * scales[s] * gains[pl.ds(start, part), :]
                ).astype(jnp.bfloat16)

    def far_arrived():
        plane_arrived(0, far)

    plane_arrived(0, near)
    if Z > 1:
        column_arrived(1)
    pair_arrived(0, near + [len(peers)])
    normalize(0, (0,))
    if not split:
        far_arrived()
        pair_arrived(0, far)
        normalize(0, range(1, Y))

    ids = jnp.concatenate([all_targets[s] for s in range(seqs)], axis=1) - me * rows
    lines = lax.broadcasted_iota(jnp.int32, (sub, tokens), 0)
    sums[...] = jnp.zeros_like(sums)

    for n, (p, i) in enumerate(bulk):
        slot = i % wides.shape[0]
        if split and (p, i) == (1, 0):
            pair_arrived(0, far)
            normalize(0, range(1, Y))
            normed[chunk:chunk + gap, :] = normed[
                pl.ds(pl.multiple_of(first_of("left"), 16), gap), :
            ]
        wide_fetch(p, i).wait()
        start = pl.multiple_of(first_of(passes[p][0][1]), 16)
        for s in range(wide // wide_sub):
            here = pl.ds(i * wide + s * wide_sub, wide_sub)
            value = jnp.dot(
                wides[slot, s * wide_sub:(s + 1) * wide_sub, :], normed[pl.ds(start, lead), :],
                preferred_element_type=jnp.float32,
            )
            logits[here, :] = logits[here, :] + value if p else value
        if n + wides.shape[0] < len(bulk):
            wide_fetch(*bulk[n + wides.shape[0]]).start()
        if split and n == 0:
            far_arrived()
        if n == min(1, len(bulk) - 1):
            for k in range(3, Z):
                column_copy(k, z).start()
        if n == min(2, len(bulk) - 1) and Z > 2:
            column_arrived(2)
        if n == min(2, len(bulk) - 1) and Z > 1:
            plane_arrived(1, near)
    if Z > 1:
        plane_arrived(1, far)

    def fold(values):
        return jnp.sum(values.reshape(sub // 8, 8, tokens), axis=0)

    events = [[] for _ in narrow]
    last_pass = len(narrow) - 1
    for k in range(3, Z):
        events[0].append((0, functools.partial(column_arrived, k)))
    for n, k in enumerate(range(2, Z)):
        events[0].append((min(tiles - 2 + n, tiles - 1), functools.partial(plane_arrived, k)))

    base = chunk if split else lead
    for p, pieces in enumerate(narrow):
        depth = sum(length for _, _, length in pieces)
        for k in sorted({piece[0] for piece in pieces}):
            if k:
                pair_arrived(k)
                normalize(k)

        def step(i, _, p=p, depth=depth, base=base):
            g = p * tiles + i
            slot = lax.rem(g, SLOTS)
            ahead = lax.rem(g + SLOTS - 1, SLOTS)

            def prefetch(q, n):
                for copy in fetches(q, n, ahead):
                    copy.start()

            n = i + SLOTS - 1
            for q in range(p, len(narrow)):
                low, high = (q - p) * tiles, (q - p + 1) * tiles
                if low > tiles - 1 + SLOTS - 1 or high <= SLOTS - 1:
                    continue
                pl.when((n >= low) & (n < high))(functools.partial(prefetch, q, n - low))
            for at, event in events[p]:
                pl.when(i == at)(event)
            for copy in fetches(p, i, slot):
                copy.wait()
            if p == last_pass:
                total, moment, chosen = sums[0], sums[1], sums[2]
            for s in range(tile // sub):
                here = pl.ds(pl.multiple_of(i * tile + s * sub, sub), sub)
                value = jnp.dot(
                    weights[slot, s * sub:(s + 1) * sub, 0:depth], normed[base:base + depth, :],
                    preferred_element_type=jnp.float32,
                )
                value = logits[here, :] + value
                if p < last_pass:
                    logits[here, :] = value
                else:
                    squashed = jnp.tanh(value * (1.0 / softcap))
                    weight = jnp.exp2(squashed * (softcap * log2e) - softcap * log2e)
                    hit = lines == ids - (i * tile + s * sub)
                    total = total + fold(weight)
                    moment = moment + fold(weight * squashed)
                    chosen = chosen + fold(jnp.where(hit, squashed, 0.0))
            if p == last_pass:
                sums[0], sums[1], sums[2] = total, moment, chosen
            return 0

        lax.fori_loop(0, tiles, step, 0)
        base += depth

    line = jnp.concatenate([
        jnp.sum(sums[0], axis=0, keepdims=True),
        softcap * jnp.sum(sums[1], axis=0, keepdims=True),
        softcap * jnp.sum(sums[2], axis=0, keepdims=True),
    ], axis=0)
    for s in range(seqs):
        stats[s] = line[:, s * own:(s + 1) * own]
    arrived[me] = stats[seq]

    square_all.wait_send()
    for k in range(1, seqs):
        target_copy(k, seq).wait_send()
    for k in range(Z):
        for j in range(len(peers)):
            plane_send(k, j).wait_send()
            pair_copy(k, j, True).wait_send()
        pair_copy(k, len(peers), True).wait_send()
        if k:
            column_copy(k, z).wait_send()

    def stat_copy(src, dst, to):
        return remote(src, dst, "stat", (), to)

    for other in others:
        to = place(*other)
        stat_copy(stats.at[to["seq"]], arrived.at[me], to).start()
    everyone = arrived.at[pl.ds(0, count - 1)]
    stat_all = stat_copy(everyone, everyone, place(*others[0]))
    stat_all.wait_recv()
    result = arrived[0]
    for i in range(1, count):
        result = result + arrived[i]
    total, moment, chosen = result[0:1], result[1:2], result[2:3]
    log_norm = softcap + jnp.log(total)
    out_ref[0:1, :] = chosen - log_norm
    out_ref[1:2, :] = log_norm - moment / total
    stat_all.wait_send()


def on_device(seqs, vocabs, hidden, norm_gain, unembed, targets):
    rows, width = unembed.shape
    own, part = hidden.shape
    Y = 2 ** ((vocabs.bit_length() - 1) // 2)
    X, Z = seqs // CORES, vocabs // Y
    sizes = {"x": X, "y": Y, "z": Z}
    count = seqs * vocabs
    tokens = seqs * own
    tile = divisor(rows, 1600)
    sub = divisor(tile, 160)
    passes = plan(Z, Y, part)
    deepest = max(sum(piece[2] for piece in pieces) for pieces in passes)
    most = max(len(pieces) for pieces in passes)
    wide = divisor(rows, 4000)
    wide_sub = divisor(wide, 160)
    spare = width + chunk_gap(passes)
    planes = X * Y
    dma = pltpu.SemaphoreType.DMA
    vmem = pl.BlockSpec(memory_space=pltpu.VMEM)
    hbm = pl.BlockSpec(memory_space=pltpu.HBM)
    out = pl.pallas_call(
        functools.partial(head_kernel, sizes, tile, sub, wide, wide_sub),
        out_shape=jax.ShapeDtypeStruct((2, own), jnp.float32),
        in_specs=[hbm] * 4,
        out_specs=vmem,
        scratch_shapes=[
            pltpu.VMEM((CORES, Z, X, Y, part, own), jnp.bfloat16),
            pltpu.VMEM((width // LANES, LANES), jnp.float32),
            pltpu.VMEM((1, own), jnp.int32),
            pltpu.VMEM((width, LANES), jnp.float32),
            pltpu.VMEM((spare, tokens), jnp.bfloat16),
            pltpu.VMEM((count, 1, own), jnp.float32),
            pltpu.VMEM((seqs, 1, own), jnp.float32),
            pltpu.VMEM((seqs, 1, own), jnp.int32),
            pltpu.VMEM((SLOTS, tile, deepest), jnp.bfloat16),
            pltpu.VMEM((min(2, rows // wide), wide, passes[0][0][2]), jnp.bfloat16),
            pltpu.VMEM((rows, tokens), jnp.float32),
            pltpu.VMEM((3, 8, tokens), jnp.float32),
            pltpu.VMEM((seqs, 3, own), jnp.float32),
            pltpu.VMEM((count, 3, own), jnp.float32),
            {
                "square": dma((2,)),
                "target": dma((2, seqs)),
                "plane": dma((2, Z, planes)),
                "column": dma((2, Z)),
                "pair": dma((2, Z, planes)),
                "stat": dma((2,)),
            },
            dma((SLOTS, most)),
            dma((2,)),
            dma((3,)),
        ],
        compiler_params=pltpu.CompilerParams(
            collective_id=0, has_side_effects=True, vmem_limit_bytes=67000000
        ),
        name="head",
    )(hidden.T, norm_gain.reshape(width // LANES, LANES), targets.reshape(1, own), unembed)
    return out[0], out[1]


def solution(mesh):
    return jax.shard_map(
        functools.partial(on_device, mesh.shape["seq"], mesh.shape["vocab"]),
        mesh=mesh,
        in_specs=(P("seq", "vocab"), P(), P(("seq", "vocab"), None), P("seq")),
        out_specs=(P("seq"), P("seq")),
        check_vma=False,
    )
```

```python
import functools

import jax
import jax.numpy as jnp
from jax import lax
from jax.experimental import pallas as pl
from jax.experimental.pallas import tpu as pltpu
from jax.sharding import PartitionSpec as P

softcap = 30.0
epsilon = 1e-06
log2e = 1.4426950408889634
CORES = 2
LANES = 128
DEPTH = 256
EARLY = 18
LATE = 22
MESH = pl.DeviceIdType.MESH


def divisor(extent, most):
    return max(n for n in range(16, most + 1, 16) if extent % n == 0)


def plan(stages, parts, part):
    chunk = parts * part
    own = part // DEPTH * DEPTH
    if parts == 2 and own and (part - own) % (LANES // 2) == 0:
        passes = [[(0, "own", own)], [(0, "rest", own)]]
        left = [(0, "left", chunk - 2 * own)]
    else:
        own = chunk // DEPTH * DEPTH
        passes = [[(0, "own", own)]]
        left = [(0, "rest", chunk - own)]
    left = [piece for piece in left if piece[2]]
    if stages > 1:
        passes.append(left + [(1, 0, chunk)])
    elif left:
        passes.append(left)
    if stages > 2:
        passes.append([(k, 0, chunk) for k in range(2, stages)])
    return passes


def chunk_gap(passes):
    return sum(piece[2] for pieces in passes for piece in pieces if piece[1] == "left")


def head_kernel(sizes, tile, sub, hidden_ref, gain_hbm, targets_hbm, unembed_ref, out_ref,
                held, gain_ref, targets_ref, gains, normed, partial, scales, all_targets, weights, logits, sums,
                stats, arrived, sems, weight_sem, load_sem):
    X, Y, Z = sizes["x"], sizes["y"], sizes["z"]
    seq, vocab = lax.axis_index("seq"), lax.axis_index("vocab")
    core = lax.rem(seq, CORES)
    x, y, z = seq // CORES, lax.rem(vocab, Y), vocab // Y
    seqs, vocabs = X * CORES, Z * Y
    count = seqs * vocabs
    me = seq * vocabs + vocab
    part, own = held.shape[4], held.shape[5]
    chunk, width, tokens = Y * part, Z * Y * part, seqs * own
    rows = unembed_ref.shape[0]
    passes = plan(Z, Y, part)
    split = [piece[1] for pieces in passes for piece in pieces].count("left") > 0
    halves = 2 if split else 1
    tiles, slots = rows // tile, weights.shape[0]
    last_pass = len(passes) - 1
    lead = passes[0][0][2]
    rest = chunk - lead

    others = [(a, b) for a in range(seqs) for b in range(vocabs) if a or b]

    def place(a, b):
        return {"seq": lax.rem(seq + a, seqs), "vocab": lax.rem(vocab + b, vocabs)}

    def device(dx=0, dy=0, dz=0, dc=0):
        return {
            "seq": lax.rem(x + dx, X) * CORES + lax.rem(core + dc, CORES),
            "vocab": lax.rem(z + dz, Z) * Y + lax.rem(y + dy, Y),
        }

    def level(k):
        return lax.rem(z - k + Z, Z)

    barrier = pltpu.get_barrier_semaphore()

    loads = [
        pltpu.make_async_copy(src, dst, load_sem.at[n])
        for n, (src, dst) in enumerate((
            (hidden_ref, held.at[core, z, x, y]), (targets_hbm, targets_ref), (gain_hbm, gain_ref)
        ))
    ]
    for load in loads:
        load.start()
    for other in others:
        pl.semaphore_signal(barrier, inc=1, device_id=place(*other), device_id_type=MESH)

    def first_of(kind):
        if not split:
            return {"own": 0, "rest": lead}.get(kind, 0)
        behind = (1 - y) * lead
        return {"own": y * rest, "rest": behind, "left": behind + lead}.get(kind, 0)

    def fetches(p, i, slot):
        start, out = 0, []
        row = pl.ds(pl.multiple_of(i * tile, tile), tile)
        for n, (k, first, length) in enumerate(passes[p]):
            column = pl.multiple_of(level(k) * chunk + first_of(first), LANES)
            out.append(pltpu.make_async_copy(
                unembed_ref.at[row, pl.ds(column, length)],
                weights.at[slot, :, pl.ds(start, length)],
                weight_sem.at[slot, n],
            ))
            start += length
        return out

    def fetch(p, i, slot):
        for copy in fetches(p, i, slot):
            copy.start()

    bulk = [(p, i) for p in range(halves) for i in range(tiles)]
    ahead = [(p, i) for p in range(len(passes)) for i in range(tiles)]
    for n in range(min(slots, len(ahead))):
        fetch(*ahead[n], n % slots)

    for load in loads:
        load.wait()
    all_targets[seq] = targets_ref[...]
    values = held[core, z, x, y].astype(jnp.float32)
    partial[me] = jnp.sum(values * values, axis=0, keepdims=True)
    pl.semaphore_wait(barrier, count - 1)

    def remote(src, dst, name, index, to):
        return pltpu.make_async_remote_copy(
            src_ref=src, dst_ref=dst, send_sem=sems[name].at[(0,) + index],
            recv_sem=sems[name].at[(1,) + index], device_id=to, device_id_type=MESH,
        )

    def square_copy(block, to):
        return remote(block, block, "square", (), to)

    square_all = square_copy(partial.at[pl.ds(0, count - 1)], place(*others[0]))

    def target_copy(k, slot):
        return remote(targets_ref, all_targets.at[slot], "target", (k,),
                      {"seq": lax.rem(seq + k, seqs), "vocab": vocab})

    peers = sorted(
        ((dx, dy) for dx in range(X) for dy in range(Y) if dx or dy),
        key=lambda d: (d[1] != 0, (d[0] != 0) + (d[1] != 0)),
    )

    def plane_copy(k, j, sx, sy):
        block = held.at[core, level(k), sx, sy]
        dx, dy = peers[j]
        return remote(block, block, "plane", (k, j), device(dx=dx, dy=dy))

    def plane_send(k, j):
        return plane_copy(k, j, x, y)

    def plane_recv(k, j):
        dx, dy = peers[j]
        return plane_copy(k, j, lax.rem(x - dx + X, X), lax.rem(y - dy + Y, Y))

    def column_copy(k, level_):
        block = held.at[core, level_, x, y]
        return remote(block, block, "column", (k,), device(dz=k))

    def pair_copy(k, j, mine):
        dx, dy = (0, 0) if j == len(peers) else peers[j]
        c = core if mine else 1 - core
        block = held.at[c, level(k), lax.rem(x - dx + X, X), lax.rem(y - dy + Y, Y)]
        return remote(block, block, "pair", (k, j), device(dc=1))

    for other in others:
        square_copy(partial.at[me], place(*other)).start()
    for k in range(1, seqs):
        target_copy(k, seq).start()

    def spread(k):
        for j in range(len(peers)):
            plane_send(k, j).start()
        pair_copy(k, len(peers), True).start()

    def column_arrived(k):
        column_copy(k, level(k)).wait_recv()
        spread(k)

    near = [j for j, d in enumerate(peers) if d[1] == 0]
    far = [j for j, d in enumerate(peers) if d[1] != 0]

    def plane_arrived(k, which=near + far):
        for j in which:
            plane_recv(k, j).wait_recv()
            pair_copy(k, j, True).start()

    def pair_arrived(k, which=near + far + [len(peers)]):
        for j in which:
            pair_copy(k, j, False).wait_recv()

    spread(0)
    for k in range(1, min(Z, 2)):
        column_copy(k, z).start()

    lanes = width // LANES
    columns = jnp.transpose(jnp.concatenate(
        [1.0 + gain_ref[...], jnp.zeros((LANES - lanes, LANES), jnp.float32)], axis=0
    ))
    for j in range(lanes):
        gains[j * LANES:(j + 1) * LANES, :] = jnp.broadcast_to(columns[:, j:j + 1], (LANES, LANES))

    plane_arrived(0, near)
    if Z > 1:
        column_arrived(1)
    square_all.wait_recv()
    for s in range(seqs):
        squares = partial[s * vocabs]
        for v in range(1, vocabs):
            squares = squares + partial[s * vocabs + v]
        scales[s] = lax.rsqrt(squares / width + epsilon)
    for k in range(2, min(Z, 3)):
        column_copy(k, z).start()
    for k in range(1, seqs):
        target_copy(k, lax.rem(seq - k + seqs, seqs)).wait_recv()

    gap = 0 if not split else rest - lead

    def normalize(k, offsets=range(Y)):
        for d in offsets:
            v = lax.rem(y + d, Y)
            for s in range(seqs):
                block = held[s % CORES, level(k), s // CORES, v].astype(jnp.float32)
                start = pl.multiple_of(level(k) * chunk + v * part, 16)
                at = pl.multiple_of(k * chunk + (gap if k else 0) + v * part, 16)
                normed[pl.ds(at, part), s * own:(s + 1) * own] = (
                    block * scales[s] * gains[pl.ds(start, part), :]
                ).astype(jnp.bfloat16)

    def far_arrived():
        plane_arrived(0, far)

    pair_arrived(0, near + [len(peers)])
    normalize(0, (0,))
    if not split:
        far_arrived()
        pair_arrived(0, far)
        normalize(0, range(1, Y))

    ids = jnp.concatenate([all_targets[s] for s in range(seqs)], axis=1) - me * rows
    lines = lax.broadcasted_iota(jnp.int32, (sub, tokens), 0)
    sums[...] = jnp.zeros_like(sums)

    for n, (p, i) in enumerate(bulk):
        slot = n % slots
        if split and (p, i) == (1, 0):
            pair_arrived(0, far)
            normalize(0, range(1, Y))
            normed[chunk:chunk + gap, :] = normed[
                pl.ds(pl.multiple_of(first_of("left"), 16), gap), :
            ]
        for copy in fetches(p, i, slot):
            copy.wait()
        start = pl.multiple_of(first_of(passes[p][0][1]), 16)
        for s in range(tile // sub):
            if Z > 1 and n == len(bulk) - 1 and s == min(EARLY, tile // sub - 1):
                last = far[-1:] if len(bulk) > 3 else near + far
                plane_arrived(1, last)
            here = pl.ds(i * tile + s * sub, sub)
            value = jnp.dot(
                weights[slot, s * sub:(s + 1) * sub, 0:lead], normed[pl.ds(start, lead), :],
                preferred_element_type=jnp.float32,
            )
            logits[here, :] = logits[here, :] + value if p else value
        if n + slots < len(ahead):
            fetch(*ahead[n + slots], slot)
        if split and n == 0:
            far_arrived()
        if n == min(1, len(bulk) - 1):
            for k in range(3, Z):
                column_copy(k, z).start()
        if n == min(2, len(bulk) - 1) and Z > 2:
            column_arrived(2)
        if n == 2 and len(bulk) > 3 and Z > 1:
            plane_arrived(1, near + far[:-1])

    def fold(values):
        return jnp.sum(values.reshape(sub // 8, 8, tokens), axis=0)

    subs = tile // sub
    first = halves
    events = {}
    for k in range(3, Z):
        events.setdefault((first, 0, 0), []).append(functools.partial(column_arrived, k))
    for k in range(2, Z):
        at = (first, tiles - 1, 0 if k < Z - 1 else min(LATE, subs - 1))
        events.setdefault(at, []).append(functools.partial(plane_arrived, k))

    base = chunk if split else lead
    for p in range(halves, len(passes)):
        pieces = passes[p]
        depth = sum(length for _, _, length in pieces)
        for k in sorted({piece[0] for piece in pieces}):
            if k:
                pair_arrived(k)
                normalize(k)

        def step(i, _, p=p, depth=depth, base=base):
            slot = lax.rem(p * tiles + i, slots)
            for copy in fetches(p, i, slot):
                copy.wait()
            if p == last_pass:
                total, moment, chosen = sums[0], sums[1], sums[2]
            for s in range(subs):
                for (q, turn, when), wanted in events.items():
                    if (q, when) == (p, s):
                        for event in wanted:
                            pl.when(i == turn)(event)
                here = pl.ds(pl.multiple_of(i * tile + s * sub, sub), sub)
                value = jnp.dot(
                    weights[slot, s * sub:(s + 1) * sub, 0:depth], normed[base:base + depth, :],
                    preferred_element_type=jnp.float32,
                )
                value = logits[here, :] + value
                if p < last_pass:
                    logits[here, :] = value
                else:
                    squashed = jnp.tanh(value * (1.0 / softcap))
                    weight = jnp.exp2(squashed * (softcap * log2e) - softcap * log2e)
                    hit = lines == ids - (i * tile + s * sub)
                    total = total + fold(weight)
                    moment = moment + fold(weight * squashed)
                    chosen = chosen + fold(jnp.where(hit, squashed, 0.0))
            if p == last_pass:
                sums[0], sums[1], sums[2] = total, moment, chosen
            for q in range(p, len(passes)):
                low = (q - p) * tiles - slots
                if low < tiles and low + tiles > 0:
                    pl.when((i >= low) & (i < low + tiles))(
                        functools.partial(fetch, q, i - low, slot)
                    )
            return 0

        lax.fori_loop(0, tiles, step, 0)
        base += depth

    line = jnp.concatenate([
        jnp.sum(sums[0], axis=0, keepdims=True),
        softcap * jnp.sum(sums[1], axis=0, keepdims=True),
        softcap * jnp.sum(sums[2], axis=0, keepdims=True),
    ], axis=0)
    for s in range(seqs):
        stats[s] = line[:, s * own:(s + 1) * own]
    arrived[me] = stats[seq]

    square_all.wait_send()
    for k in range(1, seqs):
        target_copy(k, seq).wait_send()
    for k in range(Z):
        for j in range(len(peers)):
            plane_send(k, j).wait_send()
            pair_copy(k, j, True).wait_send()
        pair_copy(k, len(peers), True).wait_send()
        if k:
            column_copy(k, z).wait_send()

    def stat_copy(src, dst, to):
        return remote(src, dst, "stat", (), to)

    for other in others:
        to = place(*other)
        stat_copy(stats.at[to["seq"]], arrived.at[me], to).start()
    everyone = arrived.at[pl.ds(0, count - 1)]
    stat_all = stat_copy(everyone, everyone, place(*others[0]))
    stat_all.wait_recv()
    result = arrived[0]
    for i in range(1, count):
        result = result + arrived[i]
    total, moment, chosen = result[0:1], result[1:2], result[2:3]
    log_norm = softcap + jnp.log(total)
    out_ref[0:1, :] = chosen - log_norm
    out_ref[1:2, :] = log_norm - moment / total
    stat_all.wait_send()


def on_device(seqs, vocabs, hidden, norm_gain, unembed, targets):
    rows, width = unembed.shape
    own, part = hidden.shape
    Y = 2 ** ((vocabs.bit_length() - 1) // 2)
    X, Z = seqs // CORES, vocabs // Y
    sizes = {"x": X, "y": Y, "z": Z}
    count = seqs * vocabs
    tokens = seqs * own
    tile = divisor(rows, 4000)
    sub = divisor(tile, 160)
    slots = min(2, rows // tile)
    passes = plan(Z, Y, part)
    deepest = max(sum(piece[2] for piece in pieces) for pieces in passes)
    most = max(len(pieces) for pieces in passes)
    spare = width + chunk_gap(passes)
    planes = X * Y
    dma = pltpu.SemaphoreType.DMA
    vmem = pl.BlockSpec(memory_space=pltpu.VMEM)
    hbm = pl.BlockSpec(memory_space=pltpu.HBM)
    out = pl.pallas_call(
        functools.partial(head_kernel, sizes, tile, sub),
        out_shape=jax.ShapeDtypeStruct((2, own), jnp.float32),
        in_specs=[hbm] * 4,
        out_specs=vmem,
        scratch_shapes=[
            pltpu.VMEM((CORES, Z, X, Y, part, own), jnp.bfloat16),
            pltpu.VMEM((width // LANES, LANES), jnp.float32),
            pltpu.VMEM((1, own), jnp.int32),
            pltpu.VMEM((width, LANES), jnp.float32),
            pltpu.VMEM((spare, tokens), jnp.bfloat16),
            pltpu.VMEM((count, 1, own), jnp.float32),
            pltpu.VMEM((seqs, 1, own), jnp.float32),
            pltpu.VMEM((seqs, 1, own), jnp.int32),
            pltpu.VMEM((slots, tile, deepest), jnp.bfloat16),
            pltpu.VMEM((rows, tokens), jnp.float32),
            pltpu.VMEM((3, 8, tokens), jnp.float32),
            pltpu.VMEM((seqs, 3, own), jnp.float32),
            pltpu.VMEM((count, 3, own), jnp.float32),
            {
                "square": dma((2,)),
                "target": dma((2, seqs)),
                "plane": dma((2, Z, planes)),
                "column": dma((2, Z)),
                "pair": dma((2, Z, planes)),
                "stat": dma((2,)),
            },
            dma((slots, most)),
            dma((3,)),
        ],
        compiler_params=pltpu.CompilerParams(
            collective_id=0, has_side_effects=True, vmem_limit_bytes=67000000
        ),
        name="head",
    )(hidden.T, norm_gain.reshape(width // LANES, LANES), targets.reshape(1, own), unembed)
    return out[0], out[1]


def solution(mesh):
    return jax.shard_map(
        functools.partial(on_device, mesh.shape["seq"], mesh.shape["vocab"]),
        mesh=mesh,
        in_specs=(P("seq", "vocab"), P(), P(("seq", "vocab"), None), P("seq")),
        out_specs=(P("seq"), P("seq")),
        check_vma=False,
    )
```
